32 devices in a mesh: ta: 4 (over y, x), xyz: 8 (over z, core).
Axes of the slice: x: 2, y: 2, z: 4, core: 2. Of those that a mesh axis runs over, the one named last changes fastest.
Arguments:
- gauge: float32 [4, 2, 3, 3, 8, 8, 1, 512], P(None, None, None, None, 'ta', 'xyz'), may hold values from -2.4 to 2.4
- clover_inverse: bfloat16 [2, 2, 6, 6, 8, 8, 1, 512], P(None, None, None, None, 'ta', 'xyz'), may hold values from -0.61 to 1
- source: float32 [2, 4, 3, 8, 8, 1, 512], P(None, None, None, 'ta', 'xyz'), may hold values from -6 to 6
- xi: float32 [2, 4, 3, 8, 8, 1, 512], P(None, None, None, 'ta', 'xyz'), may hold values from -6 to 6
- eta: float32 [2, 4, 3, 8, 8, 1, 512], P(None, None, None, 'ta', 'xyz'), may hold values from -6 to 6
- momentum: float32 [4, 2, 3, 3, 8, 8, 1, 512], P(None, None, None, None, 'ta', 'xyz'), may hold values from -6 to 6
Outputs:
- solution: float32 [2, 4, 3, 8, 8, 1, 512], P(None, None, None, 'ta', 'xyz')
- new_momentum: float32 [4, 2, 3, 3, 8, 8, 1, 512], P(None, None, None, None, 'ta', 'xyz')
The draws below stay inside these ranges and needn't reach their ends.
All inputs are finite; a program needn't handle non-finite values.
Results may differ from the reference program's by a relative error of at most 0.022.
Values may be sent and summed in bfloat16 or wider, within the bound.
No kernel may reach another device: no remote copies, remote signals or barrier semaphores. Data moves between devices by JAX's collectives and lax.ppermute only.
A program may use at most 64 MiB of HBM per device.

```python
import jax
import jax.numpy as jnp
from jax import lax

LX = 1
LY = 8
NZ = 64
ITERS = 8
NT = 8
BLOCKS = 8
NX = 8
N_XYZ = 8


def draw_clover_inverse(key, part):
    shape = (2, 2, 6, 6, NT, BLOCKS, LX, LY * NZ)
    key_diag = jax.random.fold_in(key, 11)
    key_off = jax.random.fold_in(key, 23)
    diagonal = jax.random.uniform(key_diag, shape, jnp.float32, 0.6, 1.0)
    offdiag = jnp.clip(0.15 * jax.random.normal(key_off, shape, jnp.float32), -0.6, 0.6)
    identity = jnp.eye(6, dtype=jnp.float32).reshape((1, 1, 6, 6, 1, 1, 1, 1))
    real_mask = jnp.array([1.0, 0.0], jnp.float32).reshape((1, 2, 1, 1, 1, 1, 1, 1))
    values = identity * real_mask * diagonal + (1.0 - identity) * offdiag
    return values.astype(jnp.bfloat16)


def block_scale(rng, extent, shards, smallest, top_value):
    loudness = 1.0
    for position, shards_of in shards:
        draws = jax.random.uniform(jax.random.fold_in(jax.random.fold_in(rng, 6), position), (shards_of,), jnp.float32, smallest / len(shards), top_value / len(shards))
        loudness = loudness * jnp.repeat(jnp.exp(draws), extent[position] // shards_of).reshape((-1,) + (1,) * (len(extent) - 1 - position))
    return loudness


def normal_values(key, shape, spread, bound, shards=(), kind=jnp.bfloat16):
    result = spread * jax.random.normal(key, shape, jnp.float32)
    if shards:
        result = result * block_scale(key, shape, shards, -0.22, 0.18)
    return jnp.clip(result, -bound, bound).astype(kind)


def setup_inputs(seed: int = 0) -> dict:
    key_of = jax.random.split(jax.random.key(seed), 7)
    gauge = normal_values(key_of[0], (4, 2, 3, 3, NT, BLOCKS, LX, LY * NZ), 0.4, 2.4, ((4, 4), (5, 8)), jnp.float32)
    clover_inverse = draw_clover_inverse(jax.random.fold_in(key_of[6], 71), 0)
    source = normal_values(key_of[2], (2, 4, 3, NT, BLOCKS, LX, LY * NZ), 1.0, 6.0, ((3, 4), (4, 8)), jnp.float32)
    xi = normal_values(key_of[3], (2, 4, 3, NT, BLOCKS, LX, LY * NZ), 1.0, 6.0, ((3, 4), (4, 8)), jnp.float32)
    eta = normal_values(key_of[4], (2, 4, 3, NT, BLOCKS, LX, LY * NZ), 1.0, 6.0, ((3, 4), (4, 8)), jnp.float32)
    momentum = normal_values(key_of[5], (4, 2, 3, 3, NT, BLOCKS, LX, LY * NZ), 1.0, 6.0, ((4, 4), (5, 8)), jnp.float32)
    return dict(gauge=gauge, clover_inverse=clover_inverse, source=source, xi=xi, eta=eta, momentum=momentum)


hop_scale = 0.18
step_size = 0.25


def rounded(values):
    return lax.optimization_barrier(values.astype(jnp.bfloat16)).astype(jnp.float32)


def to_grid(field):
    lead = field.shape[:-4]
    return field.reshape(lead + (NT, NX, LY, NZ))


def from_grid(field):
    lead = field.shape[:-4]
    return field.reshape(lead + (NT, N_XYZ, LX, LY * NZ))


def neighbour(field, direction, offset):
    return jnp.roll(field, -offset, axis=field.ndim - 4 + direction)


def rotate(direction, sign, real_part, imag_part):
    if direction == 0:
        return sign * real_part, sign * imag_part
    if direction == 1:
        sig_real = real_part[::-1]
        sig_imag = imag_part[::-1]
    elif direction == 2:
        sig_real = jnp.stack([imag_part[1], -imag_part[0]])
        sig_imag = jnp.stack([-real_part[1], real_part[0]])
    else:
        sig_real = jnp.stack([real_part[0], -real_part[1]])
        sig_imag = jnp.stack([imag_part[0], -imag_part[1]])
    return -sign * sig_imag, sign * sig_real


def project(direction, sign, spinor):
    inverse_sign = sign if direction == 0 else -sign
    lower_real, lower_imag = rotate(direction, inverse_sign, spinor[0, 2:], spinor[1, 2:])
    return jnp.stack([spinor[0, :2] + lower_real, spinor[1, :2] + lower_imag])


def expand(direction, sign, half_spinor):
    lower_real, lower_imag = rotate(direction, sign, half_spinor[0], half_spinor[1])
    return jnp.concatenate([half_spinor, jnp.stack([lower_real, lower_imag])], axis=1)


def colour_apply(matrix, vector):
    mat_real = matrix[0][None]
    mat_imag = matrix[1][None]
    vec_real = vector[0][:, None]
    vec_imag = vector[1][:, None]
    real_part = jnp.sum(mat_real * vec_real - mat_imag * vec_imag, axis=2)
    imag_part = jnp.sum(mat_real * vec_imag + mat_imag * vec_real, axis=2)
    return jnp.stack([real_part, imag_part])


def dagger(matrix):
    return jnp.stack([jnp.swapaxes(matrix[0], 0, 1), -jnp.swapaxes(matrix[1], 0, 1)])


def colour_product(left, right):
    left_real = left[0][:, :, None]
    left_imag = left[1][:, :, None]
    right_real = right[0][None]
    right_imag = right[1][None]
    real_part = jnp.sum(left_real * right_real - left_imag * right_imag, axis=1)
    imag_part = jnp.sum(left_real * right_imag + left_imag * right_real, axis=1)
    return jnp.stack([real_part, imag_part])


def outer_sum(left, right):
    left_real = left[0][:, :, None]
    left_imag = left[1][:, :, None]
    right_real = right[0][:, None]
    right_imag = right[1][:, None]
    real_part = jnp.sum(left_real * right_real + left_imag * right_imag, axis=0)
    imag_part = jnp.sum(left_imag * right_real - left_real * right_imag, axis=0)
    return jnp.stack([real_part, imag_part])


def traceless(force):
    real_part = 0.5 * (force[0] - jnp.swapaxes(force[0], 0, 1))
    imag_part = 0.5 * (force[1] + jnp.swapaxes(force[1], 0, 1))
    trace = (force[1, 0, 0] + force[1, 1, 1] + force[1, 2, 2]) / 3.0
    identity = jnp.eye(3, dtype=jnp.float32).reshape((3, 3) + (1,) * (force.ndim - 3))
    return jnp.stack([real_part, imag_part - identity * trace])


def clover_apply(blocks, vector):
    parts = []
    for chiral in range(2):
        piece = vector[:, 2 * chiral:2 * chiral + 2].reshape((2, 6) + vector.shape[3:])
        block_real = blocks[chiral, 0].astype(jnp.float32)
        block_imag = blocks[chiral, 1].astype(jnp.float32)
        real_part = jnp.sum(block_real * piece[0][None] - block_imag * piece[1][None], axis=1)
        imag_part = jnp.sum(block_real * piece[1][None] + block_imag * piece[0][None], axis=1)
        parts.append(jnp.stack([real_part, imag_part]).reshape((2, 2, 3) + vector.shape[3:]))
    return jnp.concatenate(parts, axis=1)


def hopping(spinor, links):
    total = jnp.zeros(spinor.shape, jnp.float32)
    for direction in range(4):
        ahead = rounded(project(direction, -1.0, neighbour(spinor, direction, 1)))
        behind = rounded(project(direction, 1.0, neighbour(spinor, direction, -1)))
        back_link = dagger(neighbour(links[direction], direction, -1))
        total = total + expand(direction, -1.0, colour_apply(links[direction], ahead))
        total = total + expand(direction, 1.0, colour_apply(back_link, behind))
    return total


def reference(gauge, clover_inverse, source, xi, eta, momentum):
    gauge = to_grid(gauge)
    clover_inverse = to_grid(clover_inverse)
    source = to_grid(source)
    xi = to_grid(xi)
    eta = to_grid(eta)
    momentum = to_grid(momentum)
    links = rounded(gauge)
    solution = clover_apply(clover_inverse, rounded(source))
    for iteration in range(ITERS):
        spinor = rounded(solution)
        solution = clover_apply(clover_inverse, rounded(source + hop_scale * hopping(spinor, links)))
    updated = []
    for direction in range(4):
        ahead_eta = neighbour(eta, direction, 1)
        ahead_xi = neighbour(xi, direction, 1)
        outer = outer_sum(expand(direction, -1.0, project(direction, -1.0, ahead_eta)), xi)
        outer = outer + outer_sum(expand(direction, 1.0, project(direction, 1.0, ahead_xi)), eta)
        force = colour_product(gauge[direction], outer)
        updated.append(momentum[direction] - step_size * traceless(force))
    return from_grid(solution), from_grid(jnp.stack(updated))
```

```python
import jax
import jax.numpy as jnp
from jax import lax
from jax.experimental import pallas as pl
from jax.experimental.pallas import tpu as pltpu
from jax.sharding import PartitionSpec as P

NZ = 64
ITERS = 8
LANES = 128
COLOURS = 3

hop_scale = 0.18
step_size = 0.25

REAL_IMAG = [(part, spin) for part in range(2) for spin in range(2)]
IN_VMEM = pl.BlockSpec(memory_space=pltpu.VMEM)


def rotation(direction, sign):
    table = {}
    for spin in range(2):
        if direction == 0:
            table[0, spin] = (0, spin, sign)
            table[1, spin] = (1, spin, sign)
            continue
        if direction == 1:
            sig_real, sig_imag = (0, 1 - spin, 1), (1, 1 - spin, 1)
        elif direction == 2:
            factor = 1 if spin == 0 else -1
            sig_real, sig_imag = (1, 1 - spin, factor), (0, 1 - spin, -factor)
        else:
            factor = 1 if spin == 0 else -1
            sig_real, sig_imag = (0, spin, factor), (1, spin, factor)
        table[0, spin] = sig_imag[:2] + (-sign * sig_imag[2],)
        table[1, spin] = sig_real[:2] + (sign * sig_real[2],)
    return table


def plus(total, term, factor=1):
    if total is None:
        return term if factor > 0 else -term
    return total + term if factor > 0 else total - term


def project(direction, sign, spinor):
    table = rotation(direction, sign if direction == 0 else -sign)
    half = {}
    for part, spin in REAL_IMAG:
        from_part, from_spin, factor = table[part, spin]
        for colour in range(COLOURS):
            half[part, spin, colour] = plus(
                spinor[part, spin, colour], spinor[from_part, from_spin + 2, colour], factor
            )
    return half


def expand_onto(total, direction, sign, half):
    table = rotation(direction, sign)
    for part, spin in REAL_IMAG:
        from_part, from_spin, factor = table[part, spin]
        for colour in range(COLOURS):
            upper = (part, spin, colour)
            lower = (part, spin + 2, colour)
            total[upper] = plus(total.get(upper), half[upper])
            total[lower] = plus(total.get(lower), half[from_part, from_spin, colour], factor)


def links_apply(link, half, dagger):
    result = {}
    for row in range(COLOURS):
        real = {spin: None for spin in range(2)}
        imag = {spin: None for spin in range(2)}
        for column in range(COLOURS):
            place = (column, row) if dagger else (row, column)
            mat_real = link(0, *place)
            mat_imag = link(1, *place)
            factor = -1 if dagger else 1
            for spin in range(2):
                vec_real = half[0, spin, column]
                vec_imag = half[1, spin, column]
                real[spin] = plus(real[spin], mat_real * vec_real)
                real[spin] = plus(real[spin], mat_imag * vec_imag, -factor)
                imag[spin] = plus(imag[spin], mat_real * vec_imag)
                imag[spin] = plus(imag[spin], mat_imag * vec_real, factor)
        for spin in range(2):
            result[0, spin, row] = real[spin]
            result[1, spin, row] = imag[spin]
    return result


def clover_apply(block, spinor):
    result = {}
    for chiral in range(2):
        for row in range(2 * COLOURS):
            real = None
            imag = None
            for column in range(2 * COLOURS):
                spin, colour = 2 * chiral + column // COLOURS, column % COLOURS
                vec_real = spinor[0, spin, colour]
                vec_imag = spinor[1, spin, colour]
                block_real = block(chiral, 0, row, column)
                block_imag = block(chiral, 1, row, column)
                real = plus(real, block_real * vec_real)
                real = plus(real, block_imag * vec_imag, -1)
                imag = plus(imag, block_real * vec_imag)
                imag = plus(imag, block_imag * vec_real)
            spin, colour = 2 * chiral + row // COLOURS, row % COLOURS
            result[0, spin, colour] = real
            result[1, spin, colour] = imag
    return result


def rounded(tile):
    return tile.astype(jnp.bfloat16).astype(jnp.float32)


HALF = [(part, spin, colour) for part in range(2) for spin in range(2) for colour in range(COLOURS)]
FULL = [(part, spin, colour) for part in range(2) for spin in range(4) for colour in range(COLOURS)]


def spinor_of(ref):
    return {key: ref[key] for key in FULL}


class Tiles:
    def __init__(self, nt, sites):
        self.rows = sites // LANES
        self.shape = (nt * self.rows, LANES)
        assert nt == 2 and self.rows * LANES == sites and LANES == 2 * NZ

    def row(self):
        return lax.broadcasted_iota(jnp.int32, self.shape, 0)

    def lane(self):
        return lax.broadcasted_iota(jnp.int32, self.shape, 1)

    def shift(self, direction, ahead):
        lane = self.lane()
        if direction == 3:
            edge = NZ - 1 if ahead else 0
            at_edge = lane % NZ == edge
            inner, outer = (LANES - 1, NZ - 1) if ahead else (1, LANES + 1 - NZ)

            def shifted(tile):
                return jnp.where(at_edge, pltpu.roll(tile, outer, 1), pltpu.roll(tile, inner, 1))

        else:
            within = self.row() % self.rows
            inner, outer = (self.shape[0] - 1, self.rows - 1) if ahead else (1, self.shape[0] + 1 - self.rows)
            at_edge = within == (self.rows - 1 if ahead else 0)
            stays = lane >= NZ if ahead else lane < NZ

            def shifted(tile):
                moved = jnp.where(at_edge, pltpu.roll(tile, outer, 0), pltpu.roll(tile, inner, 0))
                return pltpu.roll(jnp.where(stays, tile, moved), NZ, 1)

        return shifted

    def swap(self, tile):
        return pltpu.roll(tile, self.rows, 0)

    def first(self):
        return self.row() < self.rows


def keys_of(pack):
    half = len(pack) // 2
    return list(zip(pack[:half], pack[half:]))


def pack_first(tiles, face, swapped):
    first = tiles.first()
    return [jnp.where(first, face[a], swapped[b]) for a, b in keys_of(HALF)]


def pack_last(tiles, face, swapped):
    first = tiles.first()
    return [jnp.where(first, swapped[a], face[b]) for a, b in keys_of(HALF)]


def odd(axis):
    return lax.axis_index(axis) % 2 == 1


def choose(condition, yes, no):
    return jnp.where(condition, yes, no)


def ring_pairs(size, late):
    assert size % 2 == 0
    return [(i, ((i + late) ^ 1) - late if late == 0 else (((i + 1) % size) ^ 1) - 1) for i in range(size)]


def exchanged(x, axis, late):
    size = lax.axis_size(axis)
    return lax.ppermute(x, axis, [(i, j % size) for i, j in ring_pairs(size, late)])


def faces(tiles, spinor, link_of):
    behind = [links_apply(link_of(mu), project(mu, 1, spinor), True) for mu in range(2)]
    ahead = [project(mu, -1, spinor) for mu in range(2)]
    swapped_ahead = {key: tiles.swap(ahead[0][key]) for key in HALF}
    swapped_behind = {key: tiles.swap(behind[0][key]) for key in HALF}
    return ahead, behind, swapped_ahead, swapped_behind


def write_faces(tiles, spinor, link_of, sends, keeps):
    ahead, behind, swapped_ahead, swapped_behind = faces(tiles, spinor, link_of)
    x_late, t_late, t_early, x_early = sends
    x_odd, t_odd = odd("xyz"), odd("ta")
    for place, key in enumerate(HALF):
        keeps[(0,) + key] = swapped_ahead[key]
        keeps[(1,) + key] = swapped_behind[key]
        x_early[place] = choose(x_odd, ahead[1][key], behind[1][key]).astype(jnp.bfloat16)
        x_late[place] = choose(x_odd, behind[1][key], ahead[1][key]).astype(jnp.bfloat16)
    to_previous = pack_first(tiles, ahead[0], swapped_ahead)
    to_next = pack_last(tiles, behind[0], swapped_behind)
    for place, (low, high) in enumerate(zip(to_previous, to_next)):
        t_early[place] = choose(t_odd, low, high).astype(jnp.bfloat16)
        t_late[place] = choose(t_odd, high, low).astype(jnp.bfloat16)


def halo_terms(tiles, keeps, gots):
    x_late, t_late, t_early, x_early = gots
    x_odd, t_odd = odd("xyz"), odd("ta")
    first = tiles.first()
    x_ahead, x_behind, t_ahead, t_behind = {}, {}, {}, {}
    for place, key in enumerate(HALF):
        early = x_early[place].astype(jnp.float32)
        late = x_late[place].astype(jnp.float32)
        x_ahead[key] = choose(x_odd, late, early)
        x_behind[key] = choose(x_odd, early, late)
    for place, (a, b) in enumerate(keys_of(HALF)):
        early = t_early[place].astype(jnp.float32)
        late = t_late[place].astype(jnp.float32)
        from_next = choose(t_odd, late, early)
        from_previous = choose(t_odd, early, late)
        t_ahead[a] = jnp.where(first, keeps[(0,) + a], tiles.swap(from_next))
        t_ahead[b] = jnp.where(first, keeps[(0,) + b], from_next)
        t_behind[a] = jnp.where(first, from_previous, keeps[(1,) + a])
        t_behind[b] = jnp.where(first, tiles.swap(from_previous), keeps[(1,) + b])
    return [(t_ahead, t_behind), (x_ahead, x_behind)]


def in_vmem(*arrays):
    return [pltpu.with_memory_space_constraint(a, pltpu.VMEM) for a in arrays]


def kernel(body, name, outs, *ins):
    return pl.pallas_call(
        body,
        name=name,
        out_shape=tuple(outs),
        in_specs=[IN_VMEM] * len(ins),
        out_specs=(IN_VMEM,) * len(outs),
    )(*ins)


def per_device(gauge, clover_inverse, source, xi, eta, momentum):
    nt, sites = source.shape[3], source.shape[-1]
    tiles = Tiles(nt, sites)
    tile = tiles.shape

    def tiled(field):
        return field.reshape(field.shape[:-4] + tile)

    out_shapes = (source.shape, momentum.shape)
    gauge, source, xi, eta, momentum = (tiled(a) for a in (gauge, source, xi, eta, momentum))
    clover = clover_inverse.reshape(clover_inverse.shape[:4] + (nt, tiles.rows, LANES))
    clover = jnp.swapaxes(clover, 4, 5).reshape(clover_inverse.shape[:4] + tile)

    half_shape = (2, 2, COLOURS) + tile
    spinor_shape = (2, 4, COLOURS) + tile
    f32, bf16 = jnp.float32, jnp.bfloat16
    n_half = len(HALF)

    def send_shapes(extra):
        return [
            pltpu.VMEM((n_half + extra,) + tile, bf16),
            pltpu.VMEM(((n_half + extra) // 2,) + tile, bf16),
            pltpu.VMEM(((n_half + extra) // 2,) + tile, bf16),
            pltpu.VMEM((n_half + extra,) + tile, bf16),
        ]

    iterate_shapes = [pltpu.VMEM(spinor_shape, f32), pltpu.VMEM((2,) + half_shape, f32)]

    def exchange(sends):
        x_late, t_late, t_early, x_early = sends
        got = [
            exchanged(x_late, "xyz", 1),
            exchanged(t_late, "ta", 1),
            exchanged(t_early, "ta", 0),
            exchanged(x_early, "xyz", 0),
        ]
        return in_vmem(*got)

    def start(gauge_ref, clover_ref, source_ref, xi_ref, eta_ref, spinor_out, keeps, *refs):
        sends, (link_out, clover_out) = refs[:4], refs[4:]
        row = tiles.row()
        natural = (row % tiles.rows) * nt + row // tiles.rows
        for mu in range(2):
            for part in range(2):
                for i in range(COLOURS):
                    for j in range(COLOURS):
                        link_out[mu, part, i, j] = rounded(gauge_ref[mu, part, i, j])

        def block(chiral, part, i, j):
            stored = clover_ref[chiral, part, i, j].astype(f32)
            values = jnp.take_along_axis(stored, natural, axis=0)
            clover_out[chiral, part, i, j] = values
            return values

        rhs = {key: rounded(source_ref[key]) for key in FULL}
        solved = clover_apply(block, rhs)
        spinor = {}
        for key in FULL:
            spinor[key] = rounded(solved[key])
            spinor_out[key] = spinor[key]
        write_faces(tiles, spinor, lambda mu: lambda *at: link_out[(mu,) + at], sends, keeps)
        xi_here, eta_here = spinor_of(xi_ref), spinor_of(eta_ref)
        for mu in range(2):
            for half, face in enumerate((project(mu, -1, eta_here), project(mu, 1, xi_here))):
                if mu == 0:
                    swapped = {key: tiles.swap(face[key]) for key in HALF}
                    packed = pack_first(tiles, face, swapped)
                    targets = (sends[1], sends[2])
                else:
                    packed = [face[key] for key in HALF]
                    targets = (sends[0], sends[3])
                for place, values in enumerate(packed):
                    for target in targets:
                        target[(half + 1) * len(packed) + place] = values.astype(bf16)

    def local_links(gauge_ref, link_out):
        for mu in range(2):
            for part in range(2):
                for i in range(COLOURS):
                    for j in range(COLOURS):
                        link_out[mu, part, i, j] = rounded(gauge_ref[mu + 2, part, i, j])

    def local_part(spinor_ref, source_ref, link_ref, out):
        spinor = spinor_of(spinor_ref)
        total = {}
        for mu in range(2, 4):
            link = lambda *at, mu=mu: link_ref[(mu - 2,) + at]
            move = tiles.shift(mu, True)
            half = project(mu, -1, spinor)
            half = {key: move(half[key]) for key in HALF}
            expand_onto(total, mu, -1, links_apply(link, half, False))
            move = tiles.shift(mu, False)
            half = links_apply(link, project(mu, 1, spinor), True)
            half = {key: move(half[key]) for key in HALF}
            expand_onto(total, mu, 1, half)
        for key in FULL:
            out[key] = source_ref[key] + hop_scale * total[key]

    def solved_from(local_ref, keeps_ref, link_ref, clover_ref, gots):
        total = {}
        for mu, (ahead, behind) in enumerate(halo_terms(tiles, keeps_ref, gots)):
            link = lambda *at, mu=mu: link_ref[(mu,) + at]
            expand_onto(total, mu, -1, links_apply(link, ahead, False))
            expand_onto(total, mu, 1, behind)
        rhs = {key: rounded(local_ref[key] + hop_scale * total[key]) for key in FULL}
        return clover_apply(lambda *at: clover_ref[at], rhs)

    def advance(local_ref, keeps_ref, link_ref, clover_ref, *refs):
        gots, (spinor_out, keeps), sends = refs[:4], refs[4:6], refs[6:]
        solved = solved_from(local_ref, keeps_ref, link_ref, clover_ref, gots)
        spinor = {}
        for key in FULL:
            spinor[key] = rounded(solved[key])
            spinor_out[key] = spinor[key]
        write_faces(tiles, spinor, lambda mu: lambda *at: link_ref[(mu,) + at], sends, keeps)

    def finish(local_ref, keeps_ref, link_ref, clover_ref, *refs):
        gots, out = refs[:4], refs[4]
        solved = solved_from(local_ref, keeps_ref, link_ref, clover_ref, gots)
        for key in FULL:
            out[key] = solved[key]

    def momentum_update(gauge_ref, xi_ref, eta_ref, momentum_ref, *refs):
        (x_late, t_late, t_early, x_early), out = refs[:4], refs[4]
        xi_here, eta_here = spinor_of(xi_ref), spinor_of(eta_ref)
        x_odd, t_odd = odd("xyz"), odd("ta")
        first = tiles.first()
        for mu in range(4):
            ahead = []
            for half, face in enumerate((project(mu, -1, eta_here), project(mu, 1, xi_here))):
                moved = {}
                if mu == 0:
                    base = (half + 1) * (n_half // 2)
                    for place, (a, b) in enumerate(keys_of(HALF)):
                        early = t_early[base + place].astype(f32)
                        late = t_late[base + place].astype(f32)
                        got = choose(t_odd, late, early)
                        moved[a] = jnp.where(first, tiles.swap(face[a]), tiles.swap(got))
                        moved[b] = jnp.where(first, tiles.swap(face[b]), got)
                elif mu == 1:
                    base = (half + 1) * n_half
                    for place, key in enumerate(HALF):
                        early = x_early[base + place].astype(f32)
                        late = x_late[base + place].astype(f32)
                        moved[key] = choose(x_odd, late, early)
                else:
                    move = tiles.shift(mu, True)
                    moved = {key: move(face[key]) for key in HALF}
                ahead.append(moved)
            here = [project(mu, -1, xi_here), project(mu, 1, eta_here)]
            outer = {}
            for a in range(COLOURS):
                for b in range(COLOURS):
                    real = None
                    imag = None
                    for left, right in zip(ahead, here):
                        for spin in range(2):
                            left_real, left_imag = left[0, spin, a], left[1, spin, a]
                            right_real, right_imag = right[0, spin, b], right[1, spin, b]
                            real = plus(real, left_real * right_real)
                            real = plus(real, left_imag * right_imag)
                            imag = plus(imag, left_imag * right_real)
                            imag = plus(imag, left_real * right_imag, -1)
                    outer[0, a, b] = real
                    outer[1, a, b] = imag
            force = {}
            for a in range(COLOURS):
                for b in range(COLOURS):
                    real = None
                    imag = None
                    for c in range(COLOURS):
                        left_real, left_imag = gauge_ref[mu, 0, a, c], gauge_ref[mu, 1, a, c]
                        real = plus(real, left_real * outer[0, c, b])
                        real = plus(real, left_imag * outer[1, c, b], -1)
                        imag = plus(imag, left_real * outer[1, c, b])
                        imag = plus(imag, left_imag * outer[0, c, b])
                    force[0, a, b] = real
                    force[1, a, b] = imag
            trace = (force[1, 0, 0] + force[1, 1, 1] + force[1, 2, 2]) * (step_size / 3.0)
            for a in range(COLOURS):
                for b in range(COLOURS):
                    real = (0.5 * step_size) * (force[0, a, b] - force[0, b, a])
                    imag = (0.5 * step_size) * (force[1, a, b] + force[1, b, a])
                    if a == b:
                        imag = imag - trace
                    out[mu, 0, a, b] = momentum_ref[mu, 0, a, b] - real
                    out[mu, 1, a, b] = momentum_ref[mu, 1, a, b] - imag

    link_shape = (2, 2, COLOURS, COLOURS) + tile
    first_sends = send_shapes(2 * n_half)
    spinor, keeps, *rest = kernel(
        start,
        "start",
        iterate_shapes + first_sends + [pltpu.VMEM(link_shape, f32), pltpu.VMEM(clover.shape, f32)],
        *in_vmem(gauge, clover, source, xi, eta),
    )
    sends, (links_tx, clover_tiles) = rest[:4], rest[4:]
    gots = exchange(sends)
    first_gots = gots
    (links_yz,) = kernel(local_links, "local_links", [pltpu.VMEM(link_shape, f32)], *in_vmem(gauge))
    for iteration in range(ITERS):
        (local,) = kernel(
            local_part,
            "local_part",
            [pltpu.VMEM(spinor_shape, f32)],
            *in_vmem(spinor, source, links_yz),
        )
        given = in_vmem(local, keeps, links_tx, clover_tiles) + gots
        if iteration == ITERS - 1:
            (solution,) = kernel(finish, "finish", [jax.ShapeDtypeStruct(spinor_shape, f32)], *given)
            break
        spinor, keeps, *sends = kernel(advance, "advance", iterate_shapes + send_shapes(0), *given)
        gots = exchange(sends)
        if iteration == 0:
            (updated,) = kernel(
                momentum_update,
                "momentum_update",
                [jax.ShapeDtypeStruct(momentum.shape, f32)],
                *in_vmem(gauge, xi, eta, momentum),
                *first_gots,
            )
    return solution.reshape(out_shapes[0]), updated.reshape(out_shapes[1])


def solution(mesh):
    placed = (
        P(None, None, None, None, "ta", "xyz", None, None),
        P(None, None, None, None, "ta", "xyz", None, None),
        P(None, None, None, "ta", "xyz", None, None),
        P(None, None, None, "ta", "xyz", None, None),
        P(None, None, None, "ta", "xyz", None, None),
        P(None, None, None, None, "ta", "xyz", None, None),
    )
    return jax.shard_map(
        per_device,
        mesh=mesh,
        in_specs=placed,
        out_specs=(
            P(None, None, None, "ta", "xyz", None, None),
            P(None, None, None, None, "ta", "xyz", None, None),
        ),
        check_vma=False,
    )
```
